32 devices in a mesh: fsdp: 4 (over y, x), rep: 8 (over z, core).
Axes of the slice: x: 2, y: 2, z: 4, core: 2. Of those that a mesh axis runs over, the one named last changes fastest.
Arguments:
- hidden_in: bfloat16 [8192, 2048], P(('fsdp', 'rep'))
- out_grad: bfloat16 [8192, 2048], P(('fsdp', 'rep')), may hold values from -6 to 6
- attn_saved: bfloat16 [8192, 256], P(('fsdp', 'rep')), may hold values from -6 to 6
- row_lse: float32 [8192, 2], P(('fsdp', 'rep')), may hold values from 2.5 to 6
- w_qkv: bfloat16 [2048, 512], P('fsdp'), may hold values from -0.125 to 0.125
- w_out_t: bfloat16 [2048, 256], P('fsdp'), may hold values from -0.125 to 0.125
- doc_lengths: int32 [32, 4], P(('fsdp', 'rep')), may hold values from 1 to 128, 256 in all within a row
- seq_start: int32 [32], P(('fsdp', 'rep')), may hold values from 0 to 2047
Outputs:
- input_grad: bfloat16 [8192, 2048], P(('fsdp', 'rep'))
- grad_update: float32 [2048, 768], P('fsdp')
- grad_norm: float32 [], replicated
The draws below stay inside these ranges and needn't reach their ends.
Inputs may be any that keep to these rules, and one draw needn't show every extreme that they name: `doc_lengths`: each row sums to 256; the longest document of each device has exactly 128 tokens.
All inputs are finite; a program needn't handle non-finite values.
Results may differ from the reference program's by a relative error of at most 0.014.
Values may be sent and summed in bfloat16 or wider, within the bound.
No kernel may reach another device: no remote copies, remote signals or barrier semaphores. Data moves between devices by JAX's collectives and lax.ppermute only.
A program may use at most 64 MiB of HBM per device.

```python
import math
import jax
import jax.numpy as jnp
import numpy as np
from jax import lax

D = 2048
HEAD = 128
QH = 2
DOCS = 4
SEQ = 256
QW = 256
COLS = 768
TOKENS = 8192
N_FSDP = 4
N_REP = 8


def draw_hidden_in(key, part):
    base_key = jax.random.fold_in(key, 101)
    noise = jax.random.normal(jax.random.fold_in(base_key, 1), (TOKENS, D), jnp.float32)
    ramp = 0.4 * 3.0 ** (jnp.arange(D, dtype=jnp.float32) / (D - 1))
    return (noise * ramp[None, :]).astype(jnp.bfloat16)


def with_ends(drawn, stream_key, least, largest):
    longest = drawn.shape.index(max(drawn.shape))
    spots = []
    for shift in (0, 1):
        where = [jax.random.randint(jax.random.fold_in(stream_key, axis), (), 0, length) for axis, length in enumerate(drawn.shape)]
        where[longest] = (where[longest] + shift) % drawn.shape[longest]
        spots.append(tuple(where))
    return drawn.at[spots[0]].set(least).at[spots[1]].set(largest)


def steps_of(stream_key, extent, pieces, low, high):
    loudness, own = 1.0, jax.random.fold_in(stream_key, 6)
    for axis_at, parts in pieces:
        heights = jnp.exp(jax.random.uniform(jax.random.fold_in(own, axis_at), (parts,), jnp.float32, low / len(pieces), high / len(pieces)))
        loudness = loudness * jnp.repeat(heights, extent[axis_at] // parts).reshape([-1 if axis == axis_at else 1 for axis in range(len(extent))])
    return loudness


def length_profile(amount, total, reach, slope):
    loads = [(1 << 20) // math.isqrt(grade ** slope) + 1 for grade in range(2, amount + 1)]
    rest, counts = total - reach - (amount - 1), [1] * (amount - 1)
    while rest > 0:
        movable = [i for i in range(amount - 1) if counts[i] < reach]
        mass, budget = sum([loads[i] for i in movable]), rest
        for i in movable:
            more = min(reach - counts[i], max(1, budget * loads[i] // mass), rest)
            counts[i] = counts[i] + more
            rest = rest - more
    return np.array([reach] + counts)


def uneven_parts(rng, amount, total, bound, slope):
    if amount == 2:
        one = jax.random.randint(rng, (), max(1, total - bound), min(bound, total - 1) + 1)
        return jnp.stack([one, total - one])
    sizes = jnp.asarray(length_profile(amount, total, bound, slope), jnp.int32)
    couples = (amount - 1) // 2
    giver, sink = sizes[1:1 + 2 * couples:2], sizes[2:2 + 2 * couples:2]
    margin = jnp.minimum(giver - 1, bound - sink)
    moved = jax.random.randint(jax.random.fold_in(rng, 1), (couples,), 0, 1 << 20) % (margin + 1)
    sizes = sizes.at[1:1 + 2 * couples:2].set(giver - moved).at[2:2 + 2 * couples:2].set(sink + moved)
    return sizes[jax.random.permutation(jax.random.fold_in(rng, 2), amount)]


def centred(key, shape, scale, bound, cuts=(), kind=jnp.bfloat16):
    array = scale * jax.random.normal(key, shape, jnp.float32)
    if cuts:
        array = array * steps_of(key, shape, cuts, -0.22, 0.18)
    return jnp.clip(array, -bound, bound).astype(kind)


def setup_inputs(seed: int = 0) -> dict:
    key_list = jax.random.split(jax.random.key(seed), 9)
    return {
        "hidden_in": draw_hidden_in(jax.random.fold_in(key_list[8], 71), 0),
        "out_grad": centred(key_list[1], (TOKENS, D), 1.0, 6.0, ((0, 32),)),
        "attn_saved": centred(key_list[2], (TOKENS, QW), 1.0, 6.0, ((0, 32),)),
        "row_lse": jnp.clip(2.5 + 3.5 * jax.random.uniform(key_list[3], (TOKENS, QH), jnp.float32) ** steps_of(key_list[3], (TOKENS, QH), ((0, 32),), -0.2, 0.2), 2.5, 6.0),
        "w_qkv": centred(key_list[4], (D, QW + 2 * HEAD), D ** -0.5, 0.125, ((0, 4),)),
        "w_out_t": centred(key_list[5], (D, QW), D ** -0.5, 0.125, ((0, 4),)),
        "doc_lengths": jax.vmap(lambda own: uneven_parts(own, DOCS, SEQ, SEQ // 2, 2))(jax.random.split(key_list[6], (N_FSDP * N_REP))).reshape((N_FSDP * N_REP, DOCS)).astype(jnp.int32),
        "seq_start": with_ends(jax.random.randint(key_list[7], (N_FSDP * N_REP,), 0, 8 * SEQ), jax.random.fold_in(key_list[7], 1), 0, (8 * SEQ) - 1).astype(jnp.int32),
    }


def rotary(values_in, positions, turn, head_size):
    rows = values_in.shape[0]
    heads_count = values_in.shape[1] // head_size
    half_size = head_size // 2
    inverse = 1000000.0 ** (-(jnp.arange(half_size, dtype=jnp.float32) * 2.0) / head_size)
    angles = positions.astype(jnp.float32)[:, None] * inverse[None, :]
    cosine = jnp.cos(angles)[:, None, :]
    sines = jnp.sin(angles)[:, None, :]
    shaped = values_in.reshape(rows, heads_count, head_size)
    first_half = shaped[:, :, :half_size]
    second_half = shaped[:, :, half_size:]
    result = jnp.concatenate([first_half * cosine - turn * second_half * sines, second_half * cosine + turn * first_half * sines], axis=2)
    return result.reshape(rows, heads_count * head_size)

def per_device(total, inputs):
    tokens_x, grads_y, saved, lse_rows, lengths, start, w_qkv, w_out_t = inputs
    scale = 1.0 / HEAD ** 0.5
    proj = jnp.dot(tokens_x, w_qkv, preferred_element_type=jnp.float32)
    attn_grad = jnp.dot(grads_y, w_out_t, preferred_element_type=jnp.float32).astype(jnp.bfloat16)
    positions = start + jnp.arange(SEQ, dtype=jnp.int32)
    queries = rotary(proj[:, :QW], positions, 1.0, HEAD).astype(jnp.bfloat16)
    keys = rotary(proj[:, QW:QW + HEAD], positions, 1.0, HEAD).astype(jnp.bfloat16)
    values_all = proj[:, QW + HEAD:].astype(jnp.bfloat16)
    ends = jnp.cumsum(lengths)
    local_rows = jnp.arange(SEQ, dtype=jnp.int32)
    documents = lax.optimization_barrier(jnp.sum((local_rows[:, None] >= ends[None, :]).astype(jnp.int32), axis=1))
    allowed = (documents[:, None] == documents[None, :]) & (local_rows[None, :] <= local_rows[:, None])
    key_grad = jnp.zeros((SEQ, HEAD), jnp.float32)
    value_grad = jnp.zeros((SEQ, HEAD), jnp.float32)
    query_parts = []
    for head_index in range(QH):
        lower = head_index * HEAD
        query_head = queries[:, lower:lower + HEAD]
        scores = jnp.dot(query_head, keys.T, preferred_element_type=jnp.float32) * scale
        probs = jnp.where(allowed, jnp.exp(scores - lse_rows[:, head_index:head_index + 1]), 0.0)
        grad_head = attn_grad[:, lower:lower + HEAD]
        dprobs = jnp.dot(grad_head, values_all.T, preferred_element_type=jnp.float32)
        delta = lax.optimization_barrier(jnp.sum(grad_head.astype(jnp.float32) * saved[:, lower:lower + HEAD].astype(jnp.float32), axis=1, keepdims=True))
        dscores = (probs * (dprobs - delta) * scale).astype(jnp.bfloat16)
        probs_low = probs.astype(jnp.bfloat16)
        value_grad = value_grad + jnp.dot(probs_low.T, grad_head, preferred_element_type=jnp.float32)
        query_parts.append(jnp.dot(dscores, keys, preferred_element_type=jnp.float32))
        key_grad = key_grad + jnp.dot(dscores.T, query_head, preferred_element_type=jnp.float32)
    query_grad = rotary(jnp.concatenate(query_parts, axis=1), positions, -1.0, HEAD).astype(jnp.bfloat16)
    key_grad = rotary(key_grad, positions, -1.0, HEAD).astype(jnp.bfloat16)
    d_qkv = jnp.concatenate([query_grad, key_grad, value_grad.astype(jnp.bfloat16)], axis=1)
    input_grad = jnp.dot(d_qkv, w_qkv.T, preferred_element_type=jnp.float32).astype(jnp.bfloat16)
    partial_term = jnp.concatenate([jnp.dot(tokens_x.T, d_qkv, preferred_element_type=jnp.float32), jnp.dot(grads_y.T, saved, preferred_element_type=jnp.float32)], axis=1)
    rounded = lax.optimization_barrier(partial_term.astype(jnp.bfloat16)).astype(jnp.float32)
    return (total + rounded, input_grad)

def reference(hidden_in, out_grad, attn_saved, row_lse, w_qkv, w_out_t, doc_lengths, seq_start):
    groups = doc_lengths.shape[0]

    def step_fn(total, inputs):
        return per_device(total, inputs + (w_qkv, w_out_t))
    stacked = (hidden_in.reshape(groups, SEQ, D), out_grad.reshape(groups, SEQ, D), attn_saved.reshape(groups, SEQ, QW), row_lse.reshape(groups, SEQ, QH), doc_lengths, seq_start)
    grads, input_grad = lax.scan(step_fn, jnp.zeros((D, COLS), jnp.float32), stacked)
    norm_sq = jnp.sum(grads * grads)
    grad_update = grads * lax.rsqrt(norm_sq / (D * COLS) + 1e-06)
    return (input_grad.reshape(TOKENS, D), grad_update, jnp.sqrt(norm_sq))
```

```python
import functools

import jax
import jax.numpy as jnp
from jax import lax
from jax.experimental import pallas as pl
from jax.experimental.pallas import tpu as pltpu
from jax.sharding import PartitionSpec as P

HEAD = 128


VMEM = pl.BlockSpec(memory_space=pltpu.VMEM)
SMEM = pl.BlockSpec(memory_space=pltpu.SMEM)


def dot(left, right):
    return jnp.dot(left, right, preferred_element_type=jnp.float32)


def contract_rows(left, right):
    return lax.dot_general(
        left, right, (((0,), (0,)), ((), ())), preferred_element_type=jnp.float32
    )


def contract_cols(left, right):
    return lax.dot_general(
        left, right, (((1,), (1,)), ((), ())), preferred_element_type=jnp.float32
    )


def shard_cols(index, mask, width):
    return pl.ds(pl.multiple_of(jnp.bitwise_xor(index, mask) * width, width), width)


def half_cols(core, width):
    return pl.ds(pl.multiple_of(core * width, width), width)


def out_terms_kernel(shards, info, out_grad, saved, *outs):
    width = out_grad.shape[1] // shards
    half = saved.shape[1] // 2
    index, core = info[0], info[1]
    own = saved[:, half_cols(core, half)]
    other = saved[:, half_cols(1 - core, half)]
    for mask in range(shards):
        part = out_grad[:, shard_cols(index, mask, width)]
        outs[mask][...] = contract_rows(part, own).astype(jnp.bfloat16)
        outs[shards + mask][...] = contract_rows(part, other).astype(jnp.bfloat16)


def attention_kernel(shards, info, hidden, out_grad, saved, lse, cosine, sines, allowed, w_qkv,
                     w_out, *rest):
    mine = rest[: shards - 1]
    theirs = rest[shards - 1 : 2 * shards - 2]
    d_qkv = rest[2 * shards - 2]
    outs = rest[2 * shards - 1 : -2]
    proj, attn = rest[-2:]
    index, core = info[0], info[1]
    width = hidden.shape[1] // shards
    half = w_qkv.shape[1] // 2
    ohalf = w_out.shape[1] // 2
    heads = lse.shape[1]
    scale = 1.0 / HEAD**0.5
    own_cols = shard_cols(index, 0, width)
    proj[...] = dot(hidden[:, own_cols], w_qkv[...])
    attn[...] = dot(out_grad[:, own_cols], w_out[...])
    for chunks, side in ((mine, core), (theirs, 1 - core)):
        cols, ocols = half_cols(side, half), half_cols(side, ohalf)
        acc, oacc = proj[:, cols], attn[:, ocols]
        for mask in range(1, shards):
            sel = shard_cols(index, mask, width)
            chunk = chunks[mask - 1]
            acc += dot(hidden[:, sel], chunk[:, :half])
            oacc += dot(out_grad[:, sel], chunk[:, half:])
        proj[:, cols] = acc
        attn[:, ocols] = oacc
    cos, sin = cosine[...], sines[...]

    def turn(block, sign):
        return block * cos + sign * pltpu.roll(block, HEAD // 2, 1) * sin

    query_width = heads * HEAD
    keys = turn(proj[:, query_width : query_width + HEAD], 1.0).astype(jnp.bfloat16)
    values = proj[:, query_width + HEAD :].astype(jnp.bfloat16)
    see = allowed[...] > 0.0
    key_grad = jnp.zeros((hidden.shape[0], HEAD), jnp.float32)
    value_grad = jnp.zeros((hidden.shape[0], HEAD), jnp.float32)
    for head in range(heads):
        span = slice(head * HEAD, (head + 1) * HEAD)
        query = turn(proj[:, span], 1.0).astype(jnp.bfloat16)
        grad = attn[:, span].astype(jnp.bfloat16)
        scores = contract_cols(query, keys) * scale
        probs = jnp.where(see, jnp.exp(scores - lse[:, head : head + 1]), 0.0)
        dprobs = contract_cols(grad, values)
        delta = jnp.sum(
            grad.astype(jnp.float32) * saved[:, span].astype(jnp.float32), axis=1, keepdims=True
        )
        dscores = (probs * (dprobs - delta) * scale).astype(jnp.bfloat16)
        value_grad += contract_rows(probs.astype(jnp.bfloat16), grad)
        key_grad += contract_rows(dscores, query)
        d_qkv[:, span] = turn(dot(dscores, keys), -1.0).astype(jnp.bfloat16)
    d_qkv[:, query_width : query_width + HEAD] = turn(key_grad, -1.0).astype(jnp.bfloat16)
    d_qkv[:, query_width + HEAD :] = value_grad.astype(jnp.bfloat16)
    own = d_qkv[:, half_cols(core, half)]
    other = d_qkv[:, half_cols(1 - core, half)]
    for mask in range(shards):
        part = hidden[:, shard_cols(index, mask, width)]
        outs[mask][...] = contract_rows(part, own).astype(jnp.bfloat16)
        outs[shards + mask][...] = contract_rows(part, other).astype(jnp.bfloat16)


def input_kernel(shards, info, d_qkv, w_qkv, *rest):
    mine = rest[: shards - 1]
    theirs = rest[shards - 1 : 2 * shards - 2]
    out = rest[-1]
    index, core = info[0], info[1]
    width = w_qkv.shape[0]
    half = w_qkv.shape[1] // 2
    out[:, shard_cols(index, 0, width)] = contract_cols(d_qkv[...], w_qkv[...]).astype(out.dtype)
    own = d_qkv[:, half_cols(core, half)]
    other = d_qkv[:, half_cols(1 - core, half)]
    for mask in range(1, shards):
        total = contract_cols(own, mine[mask - 1][:, :half])
        total += contract_cols(other, theirs[mask - 1][:, :half])
        out[:, shard_cols(index, mask, width)] = total.astype(out.dtype)


def vmem_call(kernel, outs, name, scratch=()):
    def run(info, *args):
        return pl.pallas_call(
            kernel,
            out_shape=outs,
            in_specs=[SMEM] + [VMEM] * len(args),
            out_specs=jax.tree.map(lambda _: VMEM, outs),
            scratch_shapes=list(scratch),
            name=name,
        )(info, *args)

    return run


def arrange(pieces, place):
    stacked = jnp.stack(pieces)
    count = len(pieces)
    bit = 1
    while bit < count:
        shape = stacked.shape
        split = stacked.reshape((count // (2 * bit), 2, bit) + shape[1:])
        swapped = jnp.concatenate([split[:, 1:], split[:, :1]], axis=1)
        stacked = jnp.where((place & bit) != 0, swapped, split).reshape(shape)
        bit *= 2
    return stacked.reshape((count * pieces[0].shape[0],) + pieces[0].shape[1:])


def tree_sum(parts):
    while len(parts) > 1:
        parts = [left + right for left, right in zip(parts[::2], parts[1::2])]
    return parts[0]


def body(shards, copies, hidden_in, out_grad, attn_saved, row_lse, w_qkv, w_out_t, doc_lengths,
         seq_start):
    rows = hidden_in.shape[0]
    bf16 = jnp.bfloat16
    groups = copies // 2
    index = lax.axis_index("fsdp")
    member = lax.axis_index("rep")
    core = member % 2
    place = member // 2
    info = jnp.stack([index, core]).astype(jnp.int32)
    half, ohalf = w_qkv.shape[1] // 2, w_out_t.shape[1] // 2
    width = w_qkv.shape[0]

    def to_shard(value, mask):
        return lax.ppermute(value, "fsdp", [(i, i ^ mask) for i in range(shards)])

    def to_member(value, mask):
        return lax.ppermute(value, "rep", [(i, i ^ mask) for i in range(copies)])

    first = jnp.concatenate(
        [
            lax.dynamic_slice_in_dim(w_qkv, core * half, half, 1),
            lax.dynamic_slice_in_dim(w_out_t, core * ohalf, ohalf, 1),
        ],
        axis=1,
    )
    mine = [to_shard(first, mask) for mask in range(1, shards)]
    theirs = [to_member(chunk, 1) for chunk in mine]

    positions = seq_start[0] + jnp.arange(rows, dtype=jnp.int32)
    half_size = HEAD // 2
    inverse = 1000000.0 ** (-(jnp.arange(half_size, dtype=jnp.float32) * 2.0) / HEAD)
    angles = positions.astype(jnp.float32)[:, None] * inverse[None, :]
    cosine, sines = jnp.cos(angles), jnp.sin(angles)
    cosine = jnp.concatenate([cosine, cosine], axis=1)
    sines = jnp.concatenate([-sines, sines], axis=1)
    local = jnp.arange(rows, dtype=jnp.int32)
    ends = jnp.cumsum(doc_lengths[0])
    documents = jnp.sum((local[:, None] >= ends[None, :]).astype(jnp.int32), axis=1)
    allowed = (
        (documents[:, None] == documents[None, :]) & (local[None, :] <= local[:, None])
    ).astype(jnp.float32)

    def reduce_terms(terms):
        keep, send = terms[:shards], terms[shards:]
        total = None
        for mask in list(range(1, shards)) + [0]:
            both = keep[mask].astype(jnp.float32) + to_member(send[mask], 1).astype(jnp.float32)
            arrived = both if mask == 0 else to_shard(both.astype(bf16), mask)
            arrived = arrived.astype(jnp.float32)
            total = arrived if total is None else total + arrived
        low = total.astype(bf16)
        piece_rows = width // groups
        piece = lax.dynamic_slice_in_dim(total, place * piece_rows, piece_rows, 0)
        for mask in range(1, groups):
            away = lax.dynamic_slice_in_dim(low, (place ^ mask) * piece_rows, piece_rows, 0)
            piece = piece + to_member(away, 2 * mask).astype(jnp.float32)
        return piece

    def spread(piece):
        low = piece.astype(bf16)
        got = [low] + [to_member(low, 2 * mask) for mask in range(1, groups)]
        other = [to_member(part, 1) for part in got]
        return arrange(got, place), arrange(other, place)

    out_shape = jax.ShapeDtypeStruct((width, ohalf), bf16)
    out_terms = vmem_call(
        functools.partial(out_terms_kernel, shards), [out_shape] * (2 * shards), "out_terms"
    )(info, out_grad, attn_saved)
    qkv_shape = jax.ShapeDtypeStruct((width, half), bf16)
    results = vmem_call(
        functools.partial(attention_kernel, shards),
        [jax.ShapeDtypeStruct((rows, w_qkv.shape[1]), bf16)] + [qkv_shape] * (2 * shards),
        "attention",
        [
            pltpu.VMEM((rows, w_qkv.shape[1]), jnp.float32),
            pltpu.VMEM((rows, w_out_t.shape[1]), jnp.float32),
        ],
    )(info, hidden_in, out_grad, attn_saved, row_lse, cosine, sines, allowed, w_qkv, w_out_t,
      *mine, *theirs)
    d_qkv, qkv_terms = results[0], results[1:]
    input_grad = vmem_call(
        functools.partial(input_kernel, shards),
        jax.ShapeDtypeStruct(hidden_in.shape, bf16),
        "input_grad",
    )(info, d_qkv, w_qkv, *mine, *theirs)

    out_piece = reduce_terms(out_terms)
    qkv_piece = reduce_terms(qkv_terms)
    out_own, out_other = spread(out_piece)
    square = jnp.sum(out_piece * out_piece) + jnp.sum(qkv_piece * qkv_piece)
    square = jnp.full((1, 128), square, jnp.float32)
    qkv_own, qkv_other = spread(qkv_piece)
    line = tree_sum([square] + [to_shard(square, mask) for mask in range(1, shards)])
    norm = tree_sum([line] + [to_member(line, mask) for mask in range(1, copies)])
    norm_sq = norm[0, 0]
    whole = width * shards * (w_qkv.shape[1] + w_out_t.shape[1])
    scale = lax.rsqrt(norm_sq / whole + 1e-06)
    lower = core == 0
    grad_update = scale * jnp.concatenate(
        [
            jnp.where(lower, qkv_own, qkv_other).astype(jnp.float32),
            jnp.where(lower, qkv_other, qkv_own).astype(jnp.float32),
            jnp.where(lower, out_own, out_other).astype(jnp.float32),
            jnp.where(lower, out_other, out_own).astype(jnp.float32),
        ],
        axis=1,
    )
    return (input_grad, grad_update, jnp.sqrt(norm_sq))


def solution(mesh):
    in_specs = (
        P(("fsdp", "rep"), None),
        P(("fsdp", "rep"), None),
        P(("fsdp", "rep"), None),
        P(("fsdp", "rep"), None),
        P("fsdp", None),
        P("fsdp", None),
        P(("fsdp", "rep"), None),
        P(("fsdp", "rep")),
    )
    out_specs = (P(("fsdp", "rep"), None), P("fsdp", None), P())
    run = functools.partial(body, mesh.shape["fsdp"], mesh.shape["rep"])
    return jax.shard_map(run, mesh=mesh, in_specs=in_specs, out_specs=out_specs, check_vma=False)
```

```python
import functools

import jax
import jax.numpy as jnp
from jax import lax
from jax.experimental import pallas as pl
from jax.experimental.pallas import tpu as pltpu
from jax.sharding import PartitionSpec as P


HEAD = 128


VMEM = pl.BlockSpec(memory_space=pltpu.VMEM)
SMEM = pl.BlockSpec(memory_space=pltpu.SMEM)


def dot(left, right):
    return jnp.dot(left, right, preferred_element_type=jnp.float32)


def contract_rows(left, right):
    return lax.dot_general(
        left, right, (((0,), (0,)), ((), ())), preferred_element_type=jnp.float32
    )


def contract_cols(left, right):
    return lax.dot_general(
        left, right, (((1,), (1,)), ((), ())), preferred_element_type=jnp.float32
    )


def shard_cols(index, mask, width):
    return pl.ds(pl.multiple_of(jnp.bitwise_xor(index, mask) * width, width), width)


def half_cols(core, width):
    return pl.ds(pl.multiple_of(core * width, width), width)


def halves_kernel(info, w_qkv, w_out, out):
    half, ohalf = w_qkv.shape[1] // 2, w_out.shape[1] // 2
    out[:, :half] = w_qkv[:, half_cols(info[1], half)]
    out[:, half:] = w_out[:, half_cols(info[1], ohalf)]


def out_terms_kernel(shards, info, out_grad, saved, keep, send):
    width = out_grad.shape[1] // shards
    half = saved.shape[1] // 2
    index, core = info[0], info[1]
    own = saved[:, half_cols(core, half)]
    other = saved[:, half_cols(1 - core, half)]
    for mask in range(shards):
        part = out_grad[:, shard_cols(index, mask, width)]
        keep[mask] = contract_rows(part, own).astype(jnp.bfloat16)
        send[mask] = contract_rows(part, other).astype(jnp.bfloat16)


def attention_kernel(shards, info, hidden, out_grad, saved, lse, cosine, sines, allowed, w_qkv,
                     w_out, *rest):
    mine = rest[: shards - 1]
    theirs = rest[shards - 1 : 2 * shards - 2]
    d_qkv = rest[2 * shards - 2]
    outs = rest[2 * shards - 1 : -2]
    proj, attn = rest[-2:]
    index, core = info[0], info[1]
    width = hidden.shape[1] // shards
    half = w_qkv.shape[1] // 2
    ohalf = w_out.shape[1] // 2
    heads = lse.shape[1]
    scale = 1.0 / HEAD**0.5
    own_cols = shard_cols(index, 0, width)
    proj[...] = dot(hidden[:, own_cols], w_qkv[...])
    attn[...] = dot(out_grad[:, own_cols], w_out[...])
    for chunks, side in ((mine, core), (theirs, 1 - core)):
        cols, ocols = half_cols(side, half), half_cols(side, ohalf)
        acc, oacc = proj[:, cols], attn[:, ocols]
        for mask in range(1, shards):
            sel = shard_cols(index, mask, width)
            chunk = chunks[mask - 1]
            acc += dot(hidden[:, sel], chunk[:, :half])
            oacc += dot(out_grad[:, sel], chunk[:, half:])
        proj[:, cols] = acc
        attn[:, ocols] = oacc
    cos, sin = cosine[...], sines[...]

    def turn(block, sign):
        return block * cos + sign * pltpu.roll(block, HEAD // 2, 1) * sin

    query_width = heads * HEAD
    keys = turn(proj[:, query_width : query_width + HEAD], 1.0).astype(jnp.bfloat16)
    values = proj[:, query_width + HEAD :].astype(jnp.bfloat16)
    see = allowed[...] > 0.0
    key_grad = jnp.zeros((hidden.shape[0], HEAD), jnp.float32)
    value_grad = jnp.zeros((hidden.shape[0], HEAD), jnp.float32)
    for head in range(heads):
        span = slice(head * HEAD, (head + 1) * HEAD)
        query = turn(proj[:, span], 1.0).astype(jnp.bfloat16)
        grad = attn[:, span].astype(jnp.bfloat16)
        scores = contract_cols(query, keys) * scale
        probs = jnp.where(see, jnp.exp(scores - lse[:, head : head + 1]), 0.0)
        dprobs = contract_cols(grad, values)
        delta = jnp.sum(
            grad.astype(jnp.float32) * saved[:, span].astype(jnp.float32), axis=1, keepdims=True
        )
        dscores = (probs * (dprobs - delta) * scale).astype(jnp.bfloat16)
        value_grad += contract_rows(probs.astype(jnp.bfloat16), grad)
        key_grad += contract_rows(dscores, query)
        d_qkv[:, span] = turn(dot(dscores, keys), -1.0).astype(jnp.bfloat16)
    d_qkv[:, query_width : query_width + HEAD] = turn(key_grad, -1.0).astype(jnp.bfloat16)
    d_qkv[:, query_width + HEAD :] = value_grad.astype(jnp.bfloat16)
    own = d_qkv[:, half_cols(core, half)]
    other = d_qkv[:, half_cols(1 - core, half)]
    for mask in range(shards):
        part = hidden[:, shard_cols(index, mask, width)]
        outs[mask][...] = contract_rows(part, own).astype(jnp.bfloat16)
        outs[shards + mask][...] = contract_rows(part, other).astype(jnp.bfloat16)


def input_kernel(shards, info, d_qkv, w_qkv, *rest):
    mine = rest[: shards - 1]
    theirs = rest[shards - 1 : 2 * shards - 2]
    out = rest[-1]
    index, core = info[0], info[1]
    width = w_qkv.shape[0]
    half = w_qkv.shape[1] // 2
    out[:, shard_cols(index, 0, width)] = contract_cols(d_qkv[...], w_qkv[...]).astype(out.dtype)
    own = d_qkv[:, half_cols(core, half)]
    other = d_qkv[:, half_cols(1 - core, half)]
    for mask in range(1, shards):
        total = contract_cols(own, mine[mask - 1][:, :half])
        total += contract_cols(other, theirs[mask - 1][:, :half])
        out[:, shard_cols(index, mask, width)] = total.astype(out.dtype)


def gather_kernel(info, *rest):
    pieces, own, square = rest[:-2], rest[-2], rest[-1]
    rows = pieces[0].shape[0]
    for mask, piece in enumerate(pieces):
        spot = jnp.bitwise_xor(info[2], mask) * rows
        own[pl.ds(pl.multiple_of(spot, rows), rows), :] = piece[...]
    total = jnp.sum(jnp.square(own[...].astype(jnp.float32)))
    square[...] = jnp.full(square.shape, total, jnp.float32)


def finish_kernel(count, half, info, own, other, line, away, out, norm):
    norm_sq = line[...] + away[...]
    scale = lax.rsqrt(norm_sq / count + 1e-06)
    norm[...] = jnp.sqrt(norm_sq)
    ohalf = own.shape[1] - half
    core, lanes = info[1], scale.shape[1]
    for part, side in ((own, core), (other, 1 - core)):
        for lower in range(0, half, lanes):
            spot = pl.ds(pl.multiple_of(side * half + lower, lanes), lanes)
            out[:, spot] = part[:, lower : lower + lanes].astype(jnp.float32) * scale
        for lower in range(0, ohalf, lanes):
            spot = pl.ds(pl.multiple_of(2 * half + side * ohalf + lower, lanes), lanes)
            block = part[:, half + lower : half + lower + lanes]
            out[:, spot] = block.astype(jnp.float32) * scale


def vmem_call(kernel, outs, scratch=()):
    def run(info, *args):
        return call(info, *args)

    def call(info, *args):
        return pl.pallas_call(
            kernel,
            out_shape=outs,
            in_specs=[SMEM] + [VMEM] * len(args),
            out_specs=jax.tree.map(lambda _: VMEM, outs),
            scratch_shapes=list(scratch),
        )(info, *args)

    return run


def arrange(pieces, place):
    stacked = jnp.stack(pieces)
    count = len(pieces)
    bit = 1
    while bit < count:
        shape = stacked.shape
        split = stacked.reshape((count // (2 * bit), 2, bit) + shape[1:])
        swapped = jnp.concatenate([split[:, 1:], split[:, :1]], axis=1)
        stacked = jnp.where((place & bit) != 0, swapped, split).reshape(shape)
        bit *= 2
    return stacked.reshape((count * pieces[0].shape[0],) + pieces[0].shape[1:])


def tree_sum(parts):
    while len(parts) > 1:
        parts = [left + right for left, right in zip(parts[::2], parts[1::2])]
    return parts[0]


def body(shards, copies, hidden_in, out_grad, attn_saved, row_lse, w_qkv, w_out_t, doc_lengths,
         seq_start):
    rows = hidden_in.shape[0]
    bf16 = jnp.bfloat16
    groups = copies // 2
    index = lax.axis_index("fsdp")
    member = lax.axis_index("rep")
    core = member % 2
    place = member // 2
    info = jnp.stack([index, core, place]).astype(jnp.int32)
    half, ohalf = w_qkv.shape[1] // 2, w_out_t.shape[1] // 2
    width = w_qkv.shape[0]

    def to_shard(value, mask):
        return lax.ppermute(value, "fsdp", [(i, i ^ mask) for i in range(shards)])

    def to_member(value, mask):
        return lax.ppermute(value, "rep", [(i, i ^ mask) for i in range(copies)])

    first = vmem_call(
        halves_kernel, jax.ShapeDtypeStruct((width, half + ohalf), bf16)
    )(info, w_qkv, w_out_t)
    mine = [to_shard(first, mask) for mask in range(1, shards)]

    positions = seq_start[0] + jnp.arange(rows, dtype=jnp.int32)
    half_size = HEAD // 2
    inverse = 1000000.0 ** (-(jnp.arange(half_size, dtype=jnp.float32) * 2.0) / HEAD)
    angles = positions.astype(jnp.float32)[:, None] * inverse[None, :]
    cosine, sines = jnp.cos(angles), jnp.sin(angles)
    cosine = jnp.concatenate([cosine, cosine], axis=1)
    sines = jnp.concatenate([-sines, sines], axis=1)
    local = jnp.arange(rows, dtype=jnp.int32)
    ends = jnp.cumsum(doc_lengths[0])
    documents = jnp.sum((local[:, None] >= ends[None, :]).astype(jnp.int32), axis=1)
    allowed = (
        (documents[:, None] == documents[None, :]) & (local[None, :] <= local[:, None])
    ).astype(jnp.float32)

    out_shape = jax.ShapeDtypeStruct((shards, width, ohalf), bf16)
    out_keep, out_send = vmem_call(
        functools.partial(out_terms_kernel, shards), [out_shape] * 2
    )(info, out_grad, attn_saved)
    out_sum = out_keep.astype(jnp.float32) + to_member(out_send, 1).astype(jnp.float32)
    out_low = [out_sum[mask].astype(bf16) for mask in range(1, shards)]
    out_low, fence = lax.optimization_barrier((out_low, mine))
    theirs = [to_member(chunk, 1) for chunk in fence]
    out_got = [to_shard(low, mask + 1) for mask, low in enumerate(out_low)]

    qkv_shape = jax.ShapeDtypeStruct((width, half), bf16)
    results = vmem_call(
        functools.partial(attention_kernel, shards),
        [jax.ShapeDtypeStruct((rows, w_qkv.shape[1]), bf16)] + [qkv_shape] * (2 * shards),
        [
            pltpu.VMEM((rows, w_qkv.shape[1]), jnp.float32),
            pltpu.VMEM((rows, w_out_t.shape[1]), jnp.float32),
        ],
    )(info, hidden_in, out_grad, attn_saved, row_lse, cosine, sines, allowed, w_qkv, w_out_t,
      *fence, *theirs)
    d_qkv, keep, send = results[0], results[1 : shards + 1], results[shards + 1 :]
    input_grad = vmem_call(
        functools.partial(input_kernel, shards), jax.ShapeDtypeStruct(hidden_in.shape, bf16)
    )(info, d_qkv, w_qkv, *fence, *theirs)

    qkv_got = []
    for mask in list(range(1, shards)) + [0]:
        both = keep[mask].astype(jnp.float32) + to_member(send[mask], 1).astype(jnp.float32)
        qkv_got.append(to_shard(both.astype(bf16), mask) if mask else both)
    qkv_got, out_got, input_grad = lax.optimization_barrier((qkv_got, out_got, input_grad))
    total = jnp.concatenate(
        [
            sum(part.astype(jnp.float32) for part in qkv_got),
            sum((part.astype(jnp.float32) for part in out_got), out_sum[0]),
        ],
        axis=1,
    )
    low = total.astype(bf16)
    piece_rows = width // groups
    piece = lax.dynamic_slice_in_dim(total, place * piece_rows, piece_rows, 0)
    for mask in range(1, groups):
        away = lax.dynamic_slice_in_dim(low, (place ^ mask) * piece_rows, piece_rows, 0)
        piece = piece + to_member(away, 2 * mask).astype(jnp.float32)
    low = piece.astype(bf16)
    pieces = [low] + [to_member(low, 2 * mask) for mask in range(1, groups)]
    columns = half + ohalf
    line_shape = jax.ShapeDtypeStruct((1, 128), jnp.float32)
    if piece_rows % 16 == 0:
        own, square = vmem_call(
            gather_kernel, [jax.ShapeDtypeStruct((width, columns), bf16), line_shape]
        )(info, *pieces)
    else:
        own = arrange(pieces, place)
        square = jnp.sum(jnp.square(own.astype(jnp.float32)))
        square = jnp.full((1, 128), square, jnp.float32)
    other = to_member(own, 1)
    line = tree_sum([square] + [to_shard(square, mask) for mask in range(1, shards)])
    away = to_member(line, 1)
    grad_update, norm = vmem_call(
        functools.partial(finish_kernel, float(width * shards * 2 * columns), half),
        [jax.ShapeDtypeStruct((width, 2 * columns), jnp.float32), line_shape],
    )(info, own, other, line, away)
    return (input_grad, grad_update, norm[0, 0])


def solution(mesh):
    in_specs = (
        P(("fsdp", "rep"), None),
        P(("fsdp", "rep"), None),
        P(("fsdp", "rep"), None),
        P(("fsdp", "rep"), None),
        P("fsdp", None),
        P("fsdp", None),
        P(("fsdp", "rep"), None),
        P(("fsdp", "rep")),
    )
    out_specs = (P(("fsdp", "rep"), None), P("fsdp", None), P())

    def run(*args):
        return body(mesh.shape["fsdp"], mesh.shape["rep"], *args)

    return jax.shard_map(run, mesh=mesh, in_specs=in_specs, out_specs=out_specs, check_vma=False)
```

```python
import functools

import jax
import jax.numpy as jnp
from jax import lax
from jax.experimental import pallas as pl
from jax.experimental.pallas import tpu as pltpu
from jax.sharding import PartitionSpec as P


HEAD = 128


VMEM = pl.BlockSpec(memory_space=pltpu.VMEM)
ANY = pl.BlockSpec(memory_space=pl.ANY)
SMEM = pl.BlockSpec(memory_space=pltpu.SMEM)


def dot(left, right):
    return jnp.dot(left, right, preferred_element_type=jnp.float32)


def contract_rows(left, right):
    return lax.dot_general(
        left, right, (((0,), (0,)), ((), ())), preferred_element_type=jnp.float32
    )


def contract_cols(left, right):
    return lax.dot_general(
        left, right, (((1,), (1,)), ((), ())), preferred_element_type=jnp.float32
    )


def shard_cols(index, mask, width):
    return pl.ds(pl.multiple_of(jnp.bitwise_xor(index, mask) * width, width), width)


def half_cols(core, width):
    return pl.ds(pl.multiple_of(core * width, width), width)


def halves_kernel(info, w_qkv, w_out, out):
    half, ohalf = w_qkv.shape[1] // 2, w_out.shape[1] // 2
    out[:, :half] = w_qkv[:, half_cols(info[1], half)]
    out[:, half:] = w_out[:, half_cols(info[1], ohalf)]


def out_terms_kernel(shards, info, out_grad, saved, *rest):
    keep, send = rest[-2:]
    width = out_grad.shape[1] // shards
    half = saved.shape[1] // 2
    index, core = info[0], info[1]
    own = saved[:, half_cols(core, half)]
    other = saved[:, half_cols(1 - core, half)]
    for mask in range(shards):
        part = out_grad[:, shard_cols(index, mask, width)]
        keep[mask] = contract_rows(part, own).astype(jnp.bfloat16)
        send[mask] = contract_rows(part, other).astype(jnp.bfloat16)


def attention_kernel(shards, info, hidden, out_grad, saved, lse, cosine, sines, allowed, w_qkv,
                     w_out, *rest):
    mine = rest[: shards - 1]
    theirs = rest[shards - 1 : 2 * shards - 2]
    d_qkv = rest[2 * shards - 2]
    outs = rest[2 * shards - 1 : -2]
    proj, attn = rest[-2:]
    index, core = info[0], info[1]
    width = hidden.shape[1] // shards
    half = w_qkv.shape[1] // 2
    ohalf = w_out.shape[1] // 2
    heads = lse.shape[1]
    scale = 1.0 / HEAD**0.5
    own_cols = shard_cols(index, 0, width)
    proj[...] = dot(hidden[:, own_cols], w_qkv[...])
    attn[...] = dot(out_grad[:, own_cols], w_out[...])
    for chunks, side in ((mine, core), (theirs, 1 - core)):
        cols, ocols = half_cols(side, half), half_cols(side, ohalf)
        acc, oacc = proj[:, cols], attn[:, ocols]
        for mask in range(1, shards):
            sel = shard_cols(index, mask, width)
            chunk = chunks[mask - 1]
            acc += dot(hidden[:, sel], chunk[:, :half])
            oacc += dot(out_grad[:, sel], chunk[:, half:])
        proj[:, cols] = acc
        attn[:, ocols] = oacc
    cos, sin = cosine[...], sines[...]

    def turn(block, sign):
        return block * cos + sign * pltpu.roll(block, HEAD // 2, 1) * sin

    query_width = heads * HEAD
    keys = turn(proj[:, query_width : query_width + HEAD], 1.0).astype(jnp.bfloat16)
    values = proj[:, query_width + HEAD :].astype(jnp.bfloat16)
    see = allowed[...] > 0.0
    key_grad = jnp.zeros((hidden.shape[0], HEAD), jnp.float32)
    value_grad = jnp.zeros((hidden.shape[0], HEAD), jnp.float32)
    for head in range(heads):
        span = slice(head * HEAD, (head + 1) * HEAD)
        query = turn(proj[:, span], 1.0).astype(jnp.bfloat16)
        grad = attn[:, span].astype(jnp.bfloat16)
        scores = contract_cols(query, keys) * scale
        probs = jnp.where(see, jnp.exp(scores - lse[:, head : head + 1]), 0.0)
        dprobs = contract_cols(grad, values)
        delta = jnp.sum(
            grad.astype(jnp.float32) * saved[:, span].astype(jnp.float32), axis=1, keepdims=True
        )
        dscores = (probs * (dprobs - delta) * scale).astype(jnp.bfloat16)
        value_grad += contract_rows(probs.astype(jnp.bfloat16), grad)
        key_grad += contract_rows(dscores, query)
        d_qkv[:, span] = turn(dot(dscores, keys), -1.0).astype(jnp.bfloat16)
    d_qkv[:, query_width : query_width + HEAD] = turn(key_grad, -1.0).astype(jnp.bfloat16)
    d_qkv[:, query_width + HEAD :] = value_grad.astype(jnp.bfloat16)
    own = d_qkv[:, half_cols(core, half)]
    other = d_qkv[:, half_cols(1 - core, half)]
    for mask in range(shards):
        part = hidden[:, shard_cols(index, mask, width)]
        outs[mask][...] = contract_rows(part, own).astype(jnp.bfloat16)
        outs[shards + mask][...] = contract_rows(part, other).astype(jnp.bfloat16)


def input_kernel(shards, info, d_qkv, w_qkv, *rest):
    mine = rest[: shards - 1]
    theirs = rest[shards - 1 : 2 * shards - 2]
    out = rest[-1]
    index, core = info[0], info[1]
    width = w_qkv.shape[0]
    half = w_qkv.shape[1] // 2
    out[:, shard_cols(index, 0, width)] = contract_cols(d_qkv[...], w_qkv[...]).astype(out.dtype)
    own = d_qkv[:, half_cols(core, half)]
    other = d_qkv[:, half_cols(1 - core, half)]
    for mask in range(1, shards):
        total = contract_cols(own, mine[mask - 1][:, :half])
        total += contract_cols(other, theirs[mask - 1][:, :half])
        out[:, shard_cols(index, mask, width)] = total.astype(out.dtype)


def pack_kernel(mask, info, keep, arrived, part, out):
    rows, ohalf = keep.shape[0], part.shape[2]
    mid = part.shape[1] // 2
    total = keep[...].astype(jnp.float32) + arrived[...].astype(jnp.float32)
    out[:rows] = total.astype(out.dtype)
    out[rows:, :ohalf] = part[mask, :mid].astype(out.dtype)
    out[rows:, ohalf:] = part[mask, mid:].astype(out.dtype)


def finish_kernel(count, half, info, line, away, *rest):
    pieces, out, norm = rest[:-2], rest[-2], rest[-1]
    norm_sq = line[...] + away[...]
    scale = lax.rsqrt(norm_sq / count + 1e-06)
    norm[...] = jnp.sqrt(norm_sq)
    number, (rows, columns) = len(pieces) // 2, pieces[0].shape
    core, lanes, ohalf = info[1], scale.shape[1], columns - half
    for which, piece in enumerate(pieces):
        side = core if which < number else 1 - core
        spot = slice(None)
        if number > 1:
            row = jnp.bitwise_xor(info[2], which % number) * rows
            spot = pl.ds(pl.multiple_of(row, rows), rows)
        for lower in range(0, columns, lanes):
            start = side * half if lower < half else half + side * ohalf
            cols = pl.ds(pl.multiple_of(start + lower, lanes), lanes)
            out[spot, cols] = piece[:, lower : lower + lanes].astype(jnp.float32) * scale


def vmem_call(kernel, outs, scratch=(), waits=0):
    def run(info, *args):
        return call(info, *args)

    def call(info, *args):
        return pl.pallas_call(
            kernel,
            out_shape=outs,
            in_specs=[SMEM] + [VMEM] * (len(args) - waits) + [ANY] * waits,
            out_specs=jax.tree.map(lambda _: VMEM, outs),
            scratch_shapes=list(scratch),
        )(info, *args)

    return run


def arrange(pieces, place):
    stacked = jnp.stack(pieces)
    count = len(pieces)
    bit = 1
    while bit < count:
        shape = stacked.shape
        split = stacked.reshape((count // (2 * bit), 2, bit) + shape[1:])
        swapped = jnp.concatenate([split[:, 1:], split[:, :1]], axis=1)
        stacked = jnp.where((place & bit) != 0, swapped, split).reshape(shape)
        bit *= 2
    return stacked.reshape((count * pieces[0].shape[0],) + pieces[0].shape[1:])


def tree_sum(parts):
    while len(parts) > 1:
        parts = [left + right for left, right in zip(parts[::2], parts[1::2])]
    return parts[0]


def body(shards, copies, hidden_in, out_grad, attn_saved, row_lse, w_qkv, w_out_t, doc_lengths,
         seq_start):
    rows = hidden_in.shape[0]
    bf16 = jnp.bfloat16
    groups = copies // 2
    index = lax.axis_index("fsdp")
    member = lax.axis_index("rep")
    core = member % 2
    place = member // 2
    info = jnp.stack([index, core, place]).astype(jnp.int32)
    half, ohalf = w_qkv.shape[1] // 2, w_out_t.shape[1] // 2
    width = w_qkv.shape[0]

    def to_shard(value, mask):
        return lax.ppermute(value, "fsdp", [(i, i ^ mask) for i in range(shards)])

    def to_member(value, mask):
        return lax.ppermute(value, "rep", [(i, i ^ mask) for i in range(copies)])

    first = vmem_call(
        halves_kernel, jax.ShapeDtypeStruct((width, half + ohalf), bf16)
    )(info, w_qkv, w_out_t)
    mine = [to_shard(first, mask) for mask in range(1, shards)]

    positions = seq_start[0] + jnp.arange(rows, dtype=jnp.int32)
    half_size = HEAD // 2
    inverse = 1000000.0 ** (-(jnp.arange(half_size, dtype=jnp.float32) * 2.0) / HEAD)
    angles = positions.astype(jnp.float32)[:, None] * inverse[None, :]
    cosine, sines = jnp.cos(angles), jnp.sin(angles)
    cosine = jnp.concatenate([cosine, cosine], axis=1)
    sines = jnp.concatenate([-sines, sines], axis=1)
    local = jnp.arange(rows, dtype=jnp.int32)
    ends = jnp.cumsum(doc_lengths[0])
    documents = jnp.sum((local[:, None] >= ends[None, :]).astype(jnp.int32), axis=1)
    allowed = (
        (documents[:, None] == documents[None, :]) & (local[None, :] <= local[:, None])
    ).astype(jnp.float32)

    out_shape = jax.ShapeDtypeStruct((shards, width, ohalf), bf16)
    out_keep, out_send = vmem_call(
        functools.partial(out_terms_kernel, shards), [out_shape] * 2, waits=4
    )(info, out_grad, attn_saved, cosine, sines, allowed, row_lse)
    theirs = [to_member(chunk, 1) for chunk in mine]
    piece_rows = width // groups

    def reduce_groups(total, axis):
        low = total.astype(bf16)
        piece = lax.dynamic_slice_in_dim(total, place * piece_rows, piece_rows, axis)
        for mask in range(1, groups):
            away = lax.dynamic_slice_in_dim(low, (place ^ mask) * piece_rows, piece_rows, axis)
            piece = piece + to_member(away, 2 * mask).astype(jnp.float32)
        return piece

    out_sum = out_keep.astype(jnp.float32) + to_member(out_send, 1).astype(jnp.float32)
    out_part = reduce_groups(out_sum, 1)

    qkv_shape = jax.ShapeDtypeStruct((width, half), bf16)
    results = vmem_call(
        functools.partial(attention_kernel, shards),
        [jax.ShapeDtypeStruct((rows, w_qkv.shape[1]), bf16)] + [qkv_shape] * (2 * shards),
        [
            pltpu.VMEM((rows, w_qkv.shape[1]), jnp.float32),
            pltpu.VMEM((rows, w_out_t.shape[1]), jnp.float32),
        ],
    )(info, hidden_in, out_grad, attn_saved, row_lse, cosine, sines, allowed, w_qkv, w_out_t,
      *mine, *theirs)
    d_qkv, keep, send = results[0], results[1 : shards + 1], results[shards + 1 :]
    input_grad = vmem_call(
        functools.partial(input_kernel, shards), jax.ShapeDtypeStruct(hidden_in.shape, bf16)
    )(info, d_qkv, w_qkv, *mine, *theirs)

    mid = piece_rows // 2
    got = []
    for mask in list(range(1, shards)) + [0]:
        kind = bf16 if mask else jnp.float32
        both = vmem_call(
            functools.partial(pack_kernel, mask), jax.ShapeDtypeStruct((width + mid, half), kind)
        )(info, keep[mask], to_member(send[mask], 1), out_part)
        got.append(to_shard(both, mask) if mask else both)
    got, input_grad = lax.optimization_barrier((got, input_grad))
    total = sum(part.astype(jnp.float32) for part in got)
    out_piece = jnp.concatenate([total[width:, :ohalf], total[width:, ohalf:]], axis=0)
    piece = jnp.concatenate([reduce_groups(total[:width], 0), out_piece], axis=1)
    low = piece.astype(bf16)
    square = jnp.full((1, 128), jnp.sum(jnp.square(piece)), jnp.float32)
    own = [low] + [to_member(low, 2 * mask) for mask in range(1, groups)]
    other = [to_member(part, 1) for part in own]
    line = tree_sum([square] + [to_shard(square, mask) for mask in range(1, shards)])
    line = tree_sum([line] + [to_member(line, 2 * mask) for mask in range(1, groups)])
    away = to_member(line, 1)
    if piece_rows % 16:
        own, other = [arrange(own, place)], [arrange(other, place)]
    columns = half + ohalf
    line_shape = jax.ShapeDtypeStruct((1, 128), jnp.float32)
    grad_update, norm = vmem_call(
        functools.partial(finish_kernel, float(width * shards * 2 * columns), half),
        [jax.ShapeDtypeStruct((width, 2 * columns), jnp.float32), line_shape],
    )(info, line, away, *own, *other)
    return (input_grad, grad_update, norm[0, 0])


def solution(mesh):
    in_specs = (
        P(("fsdp", "rep"), None),
        P(("fsdp", "rep"), None),
        P(("fsdp", "rep"), None),
        P(("fsdp", "rep"), None),
        P("fsdp", None),
        P("fsdp", None),
        P(("fsdp", "rep"), None),
        P(("fsdp", "rep")),
    )
    out_specs = (P(("fsdp", "rep"), None), P("fsdp", None), P())

    def run(*args):
        return body(mesh.shape["fsdp"], mesh.shape["rep"], *args)

    return jax.shard_map(run, mesh=mesh, in_specs=in_specs, out_specs=out_specs, check_vma=False)
```

```python
import functools

import jax
import jax.numpy as jnp
from jax import lax
from jax.experimental import pallas as pl
from jax.experimental.pallas import tpu as pltpu
from jax.sharding import PartitionSpec as P


HEAD = 128


VMEM = pl.BlockSpec(memory_space=pltpu.VMEM)
ANY = pl.BlockSpec(memory_space=pl.ANY)
SMEM = pl.BlockSpec(memory_space=pltpu.SMEM)


def dot(left, right):
    return jnp.dot(left, right, preferred_element_type=jnp.float32)


def contract_rows(left, right):
    return lax.dot_general(
        left, right, (((0,), (0,)), ((), ())), preferred_element_type=jnp.float32
    )


def contract_cols(left, right):
    return lax.dot_general(
        left, right, (((1,), (1,)), ((), ())), preferred_element_type=jnp.float32
    )


def shard_cols(index, mask, width):
    return pl.ds(pl.multiple_of(jnp.bitwise_xor(index, mask) * width, width), width)


def half_cols(core, width):
    return pl.ds(pl.multiple_of(core * width, width), width)


def halves_kernel(info, w_qkv, w_out, out):
    half, ohalf = w_qkv.shape[1] // 2, w_out.shape[1] // 2
    out[:, :half] = w_qkv[:, half_cols(info[1], half)]
    out[:, half:] = w_out[:, half_cols(info[1], ohalf)]


def out_terms_kernel(shards, info, out_grad, saved, *rest):
    keep, send = rest[-2:]
    width = out_grad.shape[1] // shards
    half = saved.shape[1] // 2
    index, core = info[0], info[1]
    own = saved[:, half_cols(core, half)]
    other = saved[:, half_cols(1 - core, half)]
    for mask in range(shards):
        part = out_grad[:, shard_cols(index, mask, width)]
        keep[mask] = contract_rows(part, own).astype(jnp.bfloat16)
        send[mask] = contract_rows(part, other).astype(jnp.bfloat16)


def attention_kernel(shards, info, hidden, out_grad, saved, lse, cosine, sines, allowed, w_qkv,
                     w_out, *rest):
    mine = rest[: shards - 1]
    theirs = rest[shards - 1 : 2 * shards - 2]
    d_qkv = rest[2 * shards - 2]
    outs = rest[2 * shards - 1 : -2]
    proj, attn = rest[-2:]
    index, core = info[0], info[1]
    width = hidden.shape[1] // shards
    half = w_qkv.shape[1] // 2
    ohalf = w_out.shape[1] // 2
    heads = lse.shape[1]
    scale = 1.0 / HEAD**0.5
    own_cols = shard_cols(index, 0, width)
    proj[...] = dot(hidden[:, own_cols], w_qkv[...])
    attn[...] = dot(out_grad[:, own_cols], w_out[...])
    for chunks, side in ((mine, core), (theirs, 1 - core)):
        cols, ocols = half_cols(side, half), half_cols(side, ohalf)
        acc, oacc = proj[:, cols], attn[:, ocols]
        for mask in range(1, shards):
            sel = shard_cols(index, mask, width)
            chunk = chunks[mask - 1]
            acc += dot(hidden[:, sel], chunk[:, :half])
            oacc += dot(out_grad[:, sel], chunk[:, half:])
        proj[:, cols] = acc
        attn[:, ocols] = oacc
    cos, sin = cosine[...], sines[...]

    def turn(block, sign):
        return block * cos + sign * pltpu.roll(block, HEAD // 2, 1) * sin

    query_width = heads * HEAD
    keys = turn(proj[:, query_width : query_width + HEAD], 1.0).astype(jnp.bfloat16)
    values = proj[:, query_width + HEAD :].astype(jnp.bfloat16)
    see = allowed[...] > 0.0
    key_grad = jnp.zeros((hidden.shape[0], HEAD), jnp.float32)
    value_grad = jnp.zeros((hidden.shape[0], HEAD), jnp.float32)
    for head in range(heads):
        span = slice(head * HEAD, (head + 1) * HEAD)
        query = turn(proj[:, span], 1.0).astype(jnp.bfloat16)
        grad = attn[:, span].astype(jnp.bfloat16)
        scores = contract_cols(query, keys) * scale
        probs = jnp.where(see, jnp.exp(scores - lse[:, head : head + 1]), 0.0)
        dprobs = contract_cols(grad, values)
        delta = jnp.sum(
            grad.astype(jnp.float32) * saved[:, span].astype(jnp.float32), axis=1, keepdims=True
        )
        dscores = (probs * (dprobs - delta) * scale).astype(jnp.bfloat16)
        value_grad += contract_rows(probs.astype(jnp.bfloat16), grad)
        key_grad += contract_rows(dscores, query)
        d_qkv[:, span] = turn(dot(dscores, keys), -1.0).astype(jnp.bfloat16)
    d_qkv[:, query_width : query_width + HEAD] = turn(key_grad, -1.0).astype(jnp.bfloat16)
    d_qkv[:, query_width + HEAD :] = value_grad.astype(jnp.bfloat16)
    own = d_qkv[:, half_cols(core, half)]
    other = d_qkv[:, half_cols(1 - core, half)]
    for mask in range(shards):
        part = hidden[:, shard_cols(index, mask, width)]
        outs[mask][...] = contract_rows(part, own).astype(jnp.bfloat16)
        outs[shards + mask][...] = contract_rows(part, other).astype(jnp.bfloat16)


def input_kernel(shards, info, d_qkv, w_qkv, *rest):
    mine = rest[: shards - 1]
    theirs = rest[shards - 1 : 2 * shards - 2]
    out = rest[-1]
    index, core = info[0], info[1]
    width = w_qkv.shape[0]
    half = w_qkv.shape[1] // 2
    out[:, shard_cols(index, 0, width)] = contract_cols(d_qkv[...], w_qkv[...]).astype(out.dtype)
    own = d_qkv[:, half_cols(core, half)]
    other = d_qkv[:, half_cols(1 - core, half)]
    for mask in range(1, shards):
        total = contract_cols(own, mine[mask - 1][:, :half])
        total += contract_cols(other, theirs[mask - 1][:, :half])
        out[:, shard_cols(index, mask, width)] = total.astype(out.dtype)


def finish_kernel(count, half, info, line, away, *rest):
    pieces, out, norm = rest[:-2], rest[-2], rest[-1]
    norm_sq = line[...] + away[...]
    scale = lax.rsqrt(norm_sq / count + 1e-06)
    norm[...] = jnp.sqrt(norm_sq)
    number, (rows, columns) = len(pieces) // 2, pieces[0].shape
    core, lanes, ohalf = info[1], scale.shape[1], columns - half
    for which, piece in enumerate(pieces):
        side = core if which < number else 1 - core
        spot = slice(None)
        if number > 1:
            row = jnp.bitwise_xor(info[2], which % number) * rows
            spot = pl.ds(pl.multiple_of(row, rows), rows)
        for lower in range(0, columns, lanes):
            start = side * half if lower < half else half + side * ohalf
            cols = pl.ds(pl.multiple_of(start + lower, lanes), lanes)
            out[spot, cols] = piece[:, lower : lower + lanes].astype(jnp.float32) * scale


def vmem_call(kernel, outs, scratch=(), waits=0):
    def run(info, *args):
        return call(info, *args)

    def call(info, *args):
        return pl.pallas_call(
            kernel,
            out_shape=outs,
            in_specs=[SMEM] + [VMEM] * (len(args) - waits) + [ANY] * waits,
            out_specs=jax.tree.map(lambda _: VMEM, outs),
            scratch_shapes=list(scratch),
        )(info, *args)

    return run


def arrange(pieces, place):
    stacked = jnp.stack(pieces)
    count = len(pieces)
    bit = 1
    while bit < count:
        shape = stacked.shape
        split = stacked.reshape((count // (2 * bit), 2, bit) + shape[1:])
        swapped = jnp.concatenate([split[:, 1:], split[:, :1]], axis=1)
        stacked = jnp.where((place & bit) != 0, swapped, split).reshape(shape)
        bit *= 2
    return stacked.reshape((count * pieces[0].shape[0],) + pieces[0].shape[1:])


def tree_sum(parts):
    while len(parts) > 1:
        parts = [left + right for left, right in zip(parts[::2], parts[1::2])]
    return parts[0]


def body(shards, copies, hidden_in, out_grad, attn_saved, row_lse, w_qkv, w_out_t, doc_lengths,
         seq_start):
    rows = hidden_in.shape[0]
    bf16 = jnp.bfloat16
    groups = copies // 2
    index = lax.axis_index("fsdp")
    member = lax.axis_index("rep")
    core = member % 2
    place = member // 2
    info = jnp.stack([index, core, place]).astype(jnp.int32)
    half, ohalf = w_qkv.shape[1] // 2, w_out_t.shape[1] // 2
    width = w_qkv.shape[0]

    def to_shard(value, mask):
        return lax.ppermute(value, "fsdp", [(i, i ^ mask) for i in range(shards)])

    def to_member(value, mask):
        return lax.ppermute(value, "rep", [(i, i ^ mask) for i in range(copies)])

    first = vmem_call(
        halves_kernel, jax.ShapeDtypeStruct((width, half + ohalf), bf16)
    )(info, w_qkv, w_out_t)
    mine = [to_shard(first, mask) for mask in range(1, shards)]

    positions = seq_start[0] + jnp.arange(rows, dtype=jnp.int32)
    half_size = HEAD // 2
    inverse = 1000000.0 ** (-(jnp.arange(half_size, dtype=jnp.float32) * 2.0) / HEAD)
    angles = positions.astype(jnp.float32)[:, None] * inverse[None, :]
    cosine, sines = jnp.cos(angles), jnp.sin(angles)
    cosine = jnp.concatenate([cosine, cosine], axis=1)
    sines = jnp.concatenate([-sines, sines], axis=1)
    local = jnp.arange(rows, dtype=jnp.int32)
    ends = jnp.cumsum(doc_lengths[0])
    documents = jnp.sum((local[:, None] >= ends[None, :]).astype(jnp.int32), axis=1)
    allowed = (
        (documents[:, None] == documents[None, :]) & (local[None, :] <= local[:, None])
    ).astype(jnp.float32)

    out_shape = jax.ShapeDtypeStruct((shards, width, ohalf), bf16)
    out_keep, out_send = vmem_call(
        functools.partial(out_terms_kernel, shards), [out_shape] * 2, waits=4
    )(info, out_grad, attn_saved, cosine, sines, allowed, row_lse)
    out_sum = out_keep.astype(jnp.float32) + to_member(out_send, 1).astype(jnp.float32)
    out_low = [out_sum[mask].astype(bf16) for mask in range(1, shards)]
    out_low, fence = lax.optimization_barrier((out_low, mine))
    theirs = [to_member(chunk, 1) for chunk in fence]
    out_got = [to_shard(low, mask + 1) for mask, low in enumerate(out_low)]

    qkv_shape = jax.ShapeDtypeStruct((width, half), bf16)
    results = vmem_call(
        functools.partial(attention_kernel, shards),
        [jax.ShapeDtypeStruct((rows, w_qkv.shape[1]), bf16)] + [qkv_shape] * (2 * shards),
        [
            pltpu.VMEM((rows, w_qkv.shape[1]), jnp.float32),
            pltpu.VMEM((rows, w_out_t.shape[1]), jnp.float32),
        ],
    )(info, hidden_in, out_grad, attn_saved, row_lse, cosine, sines, allowed, w_qkv, w_out_t,
      *fence, *theirs)
    d_qkv, keep, send = results[0], results[1 : shards + 1], results[shards + 1 :]
    input_grad = vmem_call(
        functools.partial(input_kernel, shards), jax.ShapeDtypeStruct(hidden_in.shape, bf16)
    )(info, d_qkv, w_qkv, *fence, *theirs)

    qkv_got = []
    for mask in list(range(1, shards)) + [0]:
        both = keep[mask].astype(jnp.float32) + to_member(send[mask], 1).astype(jnp.float32)
        qkv_got.append(to_shard(both.astype(bf16), mask) if mask else both)
    qkv_got, out_got, input_grad = lax.optimization_barrier((qkv_got, out_got, input_grad))
    total = jnp.concatenate(
        [
            sum(part.astype(jnp.float32) for part in qkv_got),
            sum((part.astype(jnp.float32) for part in out_got), out_sum[0]),
        ],
        axis=1,
    )
    low = total.astype(bf16)
    piece_rows = width // groups
    piece = lax.dynamic_slice_in_dim(total, place * piece_rows, piece_rows, 0)
    for mask in range(1, groups):
        away = lax.dynamic_slice_in_dim(low, (place ^ mask) * piece_rows, piece_rows, 0)
        piece = piece + to_member(away, 2 * mask).astype(jnp.float32)
    low = piece.astype(bf16)
    square = jnp.full((1, 128), jnp.sum(jnp.square(piece)), jnp.float32)
    own = [low] + [to_member(low, 2 * mask) for mask in range(1, groups)]
    other = [to_member(part, 1) for part in own]
    line = tree_sum([square] + [to_shard(square, mask) for mask in range(1, shards)])
    line = tree_sum([line] + [to_member(line, 2 * mask) for mask in range(1, groups)])
    away = to_member(line, 1)
    if piece_rows % 16:
        own, other = [arrange(own, place)], [arrange(other, place)]
    columns = half + ohalf
    line_shape = jax.ShapeDtypeStruct((1, 128), jnp.float32)
    grad_update, norm = vmem_call(
        functools.partial(finish_kernel, float(width * shards * 2 * columns), half),
        [jax.ShapeDtypeStruct((width, 2 * columns), jnp.float32), line_shape],
    )(info, line, away, *own, *other)
    return (input_grad, grad_update, norm[0, 0])


def solution(mesh):
    in_specs = (
        P(("fsdp", "rep"), None),
        P(("fsdp", "rep"), None),
        P(("fsdp", "rep"), None),
        P(("fsdp", "rep"), None),
        P("fsdp", None),
        P("fsdp", None),
        P(("fsdp", "rep"), None),
        P(("fsdp", "rep")),
    )
    out_specs = (P(("fsdp", "rep"), None), P("fsdp", None), P())

    def run(*args):
        return body(mesh.shape["fsdp"], mesh.shape["rep"], *args)

    return jax.shard_map(run, mesh=mesh, in_specs=in_specs, out_specs=out_specs, check_vma=False)
```
